32 devices in a mesh: fsdp: 4 (over y, x), ctx: 4 (over z), tp: 2 (over core).
Axes of the slice: x: 2, y: 2, z: 4, core: 2. Of those that a mesh axis runs over, the one named last changes fastest.
Arguments:
- tokens: bfloat16 [12288, 1536], P(('fsdp', 'ctx')), may hold values from -6 to 6
- routes: int32 [12288, 8], P(('fsdp', 'ctx')), may hold values from 0 to 39, all different within a row
- cotangent: bfloat16 [12288, 1536], P(('fsdp', 'ctx')), may hold values from -6 to 6
- attn_gain: bfloat16 [1536], P('fsdp'), may hold values from 0.5 to 1.5
- moe_gain: bfloat16 [1536], P('fsdp'), may hold values from 0.5 to 1.5
- w_query: bfloat16 [1536, 1536], P('fsdp', 'tp'), may hold values from -0.15625 to 0.15625
- w_key: bfloat16 [1536, 512], P('fsdp', 'tp'), may hold values from -0.15625 to 0.15625
- w_value: bfloat16 [1536, 512], P('fsdp', 'tp'), may hold values from -0.15625 to 0.15625
- w_out: bfloat16 [1536, 1536], P('tp', 'fsdp'), may hold values from -1.25 to 1.25
- w_router: bfloat16 [1536, 40], P('fsdp'), may hold values from -0.078125 to 0.078125
- w_gate: bfloat16 [40, 1536, 512], P('ctx', 'fsdp', 'tp'), may hold values from -0.15625 to 0.15625
- w_up: bfloat16 [40, 1536, 512], P('ctx', 'fsdp', 'tp'), may hold values from -0.15625 to 0.15625
- w_down: bfloat16 [40, 512, 1536], P('ctx', 'tp', 'fsdp'), may hold values from -1 to 1
Outputs:
- output: bfloat16 [12288, 1536], P(('fsdp', 'ctx'))
- grad_tokens: float32 [12288, 1536], P(('fsdp', 'ctx'))
- grad_attn_gain: float32 [1536], P(('fsdp', 'ctx'))
- grad_moe_gain: float32 [1536], P(('fsdp', 'ctx'))
- grad_query: float32 [1536, 1536], P(('fsdp', 'ctx'), 'tp')
- grad_key: float32 [1536, 512], P(('fsdp', 'ctx'), 'tp')
- grad_value: float32 [1536, 512], P(('fsdp', 'ctx'), 'tp')
- grad_out: float32 [1536, 1536], P('tp', ('fsdp', 'ctx'))
- grad_router: float32 [1536, 40], P(('fsdp', 'ctx'))
- grad_gate: float32 [40, 1536, 512], P('ctx', 'fsdp', 'tp')
- grad_up: float32 [40, 1536, 512], P('ctx', 'fsdp', 'tp')
- grad_down: float32 [40, 512, 1536], P('ctx', 'tp', 'fsdp')
The draws below stay inside these ranges and needn't reach their ends.
Inputs may be any that keep to these rules, and one draw needn't show every extreme that they name: `routes`: each row names 8 different experts.
All inputs are finite; a program needn't handle non-finite values.
Results may differ from the reference program's by a relative error of at most 0.019.
Values may be sent and summed in bfloat16 or wider, within the bound.
A program may use at most 384 MiB of HBM per device.

```python
import math
import jax
import jax.numpy as jnp
from jax import lax

D = 1536
H = 24
KV = 8
HD = 64
FF = 512
EXPERTS = 40
TOPK = 8
PROMPT = 2048
CONT_LEN = 512
GROUP = 3072
TOK_DEV = 768
TOKENS = 12288
CAP = 172
N_FSDP = 4
N_CTX = 4
N_TP = 2


def level_of(rng, dims, cuts, least, top_value):
    def one(dim, blocks):
        draws = jax.random.uniform(jax.random.fold_in(jax.random.fold_in(rng, 6), dim), (blocks,), jnp.float32, least / len(cuts), top_value / len(cuts))
        return jnp.repeat(jnp.exp(draws), dims[dim] // blocks).reshape((-1,) + (1,) * (len(dims) - dim - 1))

    level = one(*cuts[0])
    for cut in cuts[1:]:
        level = level * one(*cut)
    return level


def distinct(stream_key, rows, number_of, top, lift):
    order = jax.random.permutation(jax.random.fold_in(stream_key, 1), number_of)
    boost = order
    for power in range(3):
        boost = boost * boost // number_of
    boost = boost * lift // number_of
    lots = jax.random.randint(jax.random.fold_in(stream_key, 2), (rows, number_of), 0, 4096) + boost
    sure = jax.random.permutation(jax.random.fold_in(stream_key, 3), rows)[jnp.arange(number_of) % rows]
    lots = jnp.where(jnp.arange(rows)[:, None] == sure[None, :], 1 << 14, lots)
    priority = lots * number_of + jnp.arange(number_of)
    return lax.top_k(priority.astype(jnp.int32), top)[1].astype(jnp.int32)


def gaussian(rng, extent, width, most, cuts=(), kind=jnp.bfloat16):
    factor_of = level_of(rng, extent, cuts, -0.22, 0.18) if cuts else 1.0
    values = jax.random.normal(rng, extent, jnp.float32) * width * factor_of
    return jnp.minimum(jnp.maximum(values, -most), most).astype(kind)


def setup_inputs(seed: int = 0) -> dict:
    splits = jax.random.split(jax.random.key(seed), 14)
    tokens = gaussian(splits[0], (TOKENS, D), 1.0, 6.0, ((0, 16),))
    routes = distinct(splits[1], TOKENS, EXPERTS, TOPK, 1638)
    cotangent = gaussian(splits[2], (TOKENS, D), 1.0, 6.0, ((0, 16),))
    attn_gain = jnp.clip(1.0 + 0.1 * jax.random.normal(splits[3], (D,), jnp.float32), 0.5, 1.5).astype(jnp.bfloat16)
    moe_gain = jnp.clip(1.0 + 0.1 * jax.random.normal(splits[4], (D,), jnp.float32), 0.5, 1.5).astype(jnp.bfloat16)
    w_query = gaussian(splits[5], (D, H * HD), D ** -0.5, 0.15625, ((0, 4), (1, 2)))
    w_key = gaussian(splits[6], (D, KV * HD), D ** -0.5, 0.15625, ((0, 4), (1, 2)))
    w_value = gaussian(splits[7], (D, KV * HD), D ** -0.5, 0.15625, ((0, 4), (1, 2)))
    w_out = gaussian(splits[8], (H * HD, D), (H * HD // 64) ** -0.5, 1.25, ((0, 2), (1, 4)))
    w_router = gaussian(splits[9], (D, EXPERTS), (4 * D) ** -0.5, 0.078125, ((0, 4),))
    w_gate = gaussian(splits[10], (EXPERTS, D, FF), D ** -0.5, 0.15625, ((0, 4), (1, 4), (2, 2)))
    w_up = gaussian(splits[11], (EXPERTS, D, FF), D ** -0.5, 0.15625, ((0, 4), (1, 4), (2, 2)))
    w_down = gaussian(splits[12], (EXPERTS, FF, D), (FF // 16) ** -0.5, 1.0, ((0, 4), (1, 2), (2, 4)))
    return {"tokens": tokens, "routes": routes, "cotangent": cotangent, "attn_gain": attn_gain, "moe_gain": moe_gain, "w_query": w_query, "w_key": w_key, "w_value": w_value, "w_out": w_out, "w_router": w_router, "w_gate": w_gate, "w_up": w_up, "w_down": w_down}


@jax.custom_vjp
def low(v):
    return lax.optimization_barrier(v.astype(jnp.bfloat16)).astype(jnp.float32)

@jax.custom_vjp
def low_back(v):
    return v

def low_keep(v):
    return (low(v), None)

def low_pass(kept, grad):
    return (grad,)

def back_keep(v):
    return (v, None)

def back_low(kept, grad):
    return (low(grad),)
low.defvjp(low_keep, low_pass)
low_back.defvjp(back_keep, back_low)
HIGH = lax.Precision.HIGHEST
norm_eps = 1e-06
rope_base = 10000.0

def rms_norm(values, gain):
    inverse = lax.rsqrt(lax.optimization_barrier(jnp.mean(values * values, axis=-1, keepdims=True)) + norm_eps)
    return values * inverse * gain

def layout(count):
    index = jnp.arange(count, dtype=jnp.int32)
    after = index - PROMPT
    segment = jnp.where(index < PROMPT, 0, 1 + after // CONT_LEN)
    position = jnp.where(index < PROMPT, index, PROMPT + after % CONT_LEN)
    return (index, segment, position)

def rotation(position):
    halfway = HD // 2
    freq = rope_base ** (-jnp.arange(halfway, dtype=jnp.float32) * 2.0 / HD)
    angle = position.astype(jnp.float32)[:, None] * freq[None, :]
    return (jnp.cos(angle)[:, None, :], jnp.sin(angle)[:, None, :])

def rotate(values, cosine, sine):
    halfway = HD // 2
    former = values[..., :halfway]
    latter = values[..., halfway:]
    return jnp.concatenate([former * cosine - latter * sine, latter * cosine + former * sine], axis=-1)

def slot_table(routes_group):
    picks = routes_group.reshape(N_CTX, TOK_DEV * TOPK)
    flags = (picks[:, :, None] == jnp.arange(EXPERTS, dtype=jnp.int32)).astype(jnp.int32)
    ranks = lax.optimization_barrier(jnp.sum((jnp.cumsum(flags, axis=1) - 1) * flags, axis=2))
    blocks = jnp.arange(N_CTX, dtype=jnp.int32)[:, None]
    target = jnp.where(ranks < CAP, picks * (N_CTX * CAP) + blocks * CAP + ranks, EXPERTS * N_CTX * CAP)
    source = blocks * (TOK_DEV * TOPK) + jnp.arange(TOK_DEV * TOPK, dtype=jnp.int32)[None, :]
    table = jnp.full((EXPERTS * N_CTX * CAP,), -1, jnp.int32)
    table = table.at[target.reshape(-1)].set(source.reshape(-1), mode='drop')
    return table.reshape(EXPERTS, N_CTX * CAP)

def group_forward(tokens, table, routes, weights):
    attn_gain, moe_gain, w_query, w_key, w_value, w_out, w_router, w_gate, w_up, w_down = weights
    index, segment, position = layout(GROUP)
    cosine, sine = rotation(position)
    normed = low(rms_norm(tokens, attn_gain))
    query_pre = jnp.dot(normed, w_query, precision=HIGH).reshape(GROUP, H, HD)
    key_pre = jnp.dot(normed, w_key, precision=HIGH).reshape(GROUP, KV, HD)
    values = low(low_back(jnp.dot(normed, w_value, precision=HIGH))).reshape(GROUP, KV, HD)
    queries = low(rotate(low_back(query_pre), cosine, sine)).reshape(GROUP, KV, H // KV, HD)
    keys = low(rotate(low_back(key_pre), cosine, sine))
    block = math.gcd(GROUP, 512)
    scale = HD ** (-0.5)

    def attend(start):
        rows_now = lax.dynamic_slice_in_dim(queries, start, block, 0)
        row_index = lax.dynamic_slice_in_dim(index, start, block, 0)
        row_segment = lax.dynamic_slice_in_dim(segment, start, block, 0)
        allowed = (index[None, :] <= row_index[:, None]) & ((segment[None, :] == 0) | (segment[None, :] == row_segment[:, None]))
        scores = low_back(jnp.einsum('qjrd,kjd->qjrk', rows_now, keys, precision=HIGH)) * scale
        scores = jnp.where(allowed[:, None, None, :], scores, -1e+30)
        probs = low(jax.nn.softmax(scores, axis=-1))
        return jnp.einsum('qjrk,kjd->qjrd', probs, values, precision=HIGH).reshape(block, H * HD)
    starts = jnp.arange(GROUP // block, dtype=jnp.int32) * block
    mixed = lax.map(jax.checkpoint(attend), starts).reshape(GROUP, H * HD)
    mixed = low(low_back(mixed))
    hidden = tokens + low_back(jnp.dot(mixed, w_out, precision=HIGH))
    normed_two = low(rms_norm(hidden, moe_gain))
    logits = low_back(jnp.dot(normed_two, w_router, precision=HIGH))
    chosen = jnp.take_along_axis(logits, routes, axis=1)
    gates = jax.nn.softmax(chosen, axis=-1).reshape(-1)
    portion = FF // N_TP

    def expert(total, item):
        source, gate_w, up_w, down_w = item
        filled = source >= 0
        safe = jnp.where(filled, source, 0)
        owner = safe // TOPK
        weight = jnp.where(filled, gates[safe], 0.0)
        inputs = low_back(normed_two[owner])
        summed = jnp.zeros((N_CTX * CAP, D), jnp.float32)
        for part_index in range(N_TP):
            lower = part_index * portion
            gate_pre = low_back(jnp.dot(inputs, gate_w[:, lower:lower + portion], precision=HIGH))
            up_pre = low_back(jnp.dot(inputs, up_w[:, lower:lower + portion], precision=HIGH))
            active = low(jax.nn.silu(gate_pre) * up_pre)
            summed = summed + jnp.dot(active, down_w[lower:lower + portion], precision=HIGH)
        result = low_back(low(summed))
        total = total.at[owner].add(weight[:, None] * result)
        return (total, None)
    start_total = jnp.zeros((GROUP, D), jnp.float32)
    moe, unused = lax.scan(jax.checkpoint(expert), start_total, (table, w_gate, w_up, w_down))
    return hidden + low_back(moe)

def reference(tokens, routes, cotangent, attn_gain, moe_gain, w_query, w_key, w_value, w_out, w_router, w_gate, w_up, w_down):
    grouped_routes = routes.reshape(N_FSDP, GROUP, TOPK)
    tables = lax.map(slot_table, grouped_routes)

    def forward(tokens_f, *weights):

        def one_group(item):
            return group_forward(item[0], item[1], item[2], weights)
        result = lax.map(jax.checkpoint(one_group), (tokens_f.reshape(N_FSDP, GROUP, D), tables, grouped_routes))
        return result.reshape(TOKENS, D)
    inputs = [array.astype(jnp.float32) for array in (tokens, attn_gain, moe_gain, w_query, w_key, w_value, w_out, w_router, w_gate, w_up, w_down)]
    output, pull = jax.vjp(forward, *inputs)
    grads = pull(cotangent.astype(jnp.float32))
    return (output.astype(jnp.bfloat16), grads[0], grads[1], grads[2], grads[3], grads[4], grads[5], grads[6], grads[7], grads[8], grads[9], grads[10])
```

```python
import jax
import jax.numpy as jnp
from jax import lax
from jax.sharding import PartitionSpec as P

H = 24
KV = 8
HD = 64
TOPK = 8
PROMPT = 2048
CONT_LEN = 512


norm_eps = 1e-06
rope_base = 10000.0


def rotation(position):
    halfway = HD // 2
    freq = rope_base ** (-jnp.arange(halfway, dtype=jnp.float32) * 2.0 / HD)
    angle = position.astype(jnp.float32)[:, None] * freq[None, :]
    return (jnp.cos(angle)[:, None, :], jnp.sin(angle)[:, None, :])


def rotate(values, cosine, sine):
    halfway = HD // 2
    former = values[..., :halfway]
    latter = values[..., halfway:]
    return jnp.concatenate(
        [former * cosine - latter * sine, latter * cosine + former * sine], axis=-1
    )


def over_rows(left, right):
    return lax.dot_general(
        left, right, (((0,), (0,)), ((), ())), preferred_element_type=jnp.float32
    )


def over_cols(left, right):
    return lax.dot_general(
        left, right, (((1,), (1,)), ((), ())), preferred_element_type=jnp.float32
    )


def gather_spread(rows):
    part = rows.shape[0] // lax.axis_size("tp")
    mine = lax.dynamic_slice_in_dim(rows, lax.axis_index("tp") * part, part)
    return lax.all_gather(mine, ("ctx", "tp"), axis=0, tiled=True)


def sum_to_owner(terms):
    piece = lax.psum_scatter(
        terms.astype(jnp.bfloat16), ("ctx", "tp"), scatter_dimension=0, tiled=True
    )
    return lax.all_gather(piece, "tp", axis=0, tiled=True).astype(jnp.float32)


def on_device(
    tokens,
    routes,
    cotangent,
    attn_gain,
    moe_gain,
    w_query,
    w_key,
    w_value,
    w_out,
    w_router,
    w_gate,
    w_up,
    w_down,
):
    count, width = tokens.shape
    spread = lax.axis_size("ctx")
    place = lax.axis_index("ctx")
    tp_size = lax.axis_size("tp")
    group = count * spread
    query_cols, key_cols = w_query.shape[1], w_key.shape[1]
    qkv_full = lax.all_gather(
        jnp.concatenate([w_query, w_key, w_value], axis=1), "fsdp", axis=0, tiled=True
    )
    query_full = qkv_full[:, :query_cols]
    key_full = qkv_full[:, query_cols : query_cols + key_cols]
    value_full = qkv_full[:, query_cols + key_cols :]
    attn_scale = lax.all_gather(attn_gain, "fsdp", axis=0, tiled=True)
    moe_scale = lax.all_gather(moe_gain, "fsdp", axis=0, tiled=True)
    routes_all = lax.all_gather(routes, "ctx", axis=0)
    out_full = lax.all_gather(w_out, "fsdp", axis=1, tiled=True)
    router_full = lax.all_gather(w_router, "fsdp", axis=0, tiled=True)
    cotangent_all = gather_spread(cotangent).reshape(spread, count, width)
    hidden_units = w_gate.shape[2]
    joined = jnp.concatenate([w_gate, w_up, jnp.swapaxes(w_down, 1, 2)], axis=2)
    joined_full = lax.all_gather(joined, "fsdp", axis=1, tiled=True)
    gate_up_full = joined_full[:, :, : 2 * hidden_units]
    down_full = joined_full[:, :, 2 * hidden_units :]
    index_all = jnp.arange(group, dtype=jnp.int32)
    segment_all = jnp.where(index_all < PROMPT, 0, 1 + (index_all - PROMPT) // CONT_LEN)
    position_all = jnp.where(
        index_all < PROMPT, index_all, PROMPT + (index_all - PROMPT) % CONT_LEN
    )
    first_row = place * count
    row_index = lax.dynamic_slice_in_dim(index_all, first_row, count)
    row_segment = lax.dynamic_slice_in_dim(segment_all, first_row, count)
    row_position = lax.dynamic_slice_in_dim(position_all, first_row, count)
    allowed = (index_all[None, :] <= row_index[:, None]) & (
        (segment_all[None, :] == 0) | (segment_all[None, :] == row_segment[:, None])
    )
    cosine, sine = rotation(row_position)
    scale = HD ** (-0.5)
    ratio = H // KV
    kv_local = key_cols // HD

    experts = w_router.shape[1]
    capacity = max(tp_size, 9 * count * TOPK // (8 * experts) // tp_size * tp_size)
    padded = -(-capacity // 16) * 16
    local_experts = experts // spread
    first_expert = place * local_experts
    expert_ids = jnp.arange(experts, dtype=jnp.int32)
    local_ids = first_expert + jnp.arange(local_experts, dtype=jnp.int32)
    routes_t = jnp.swapaxes(routes_all, 1, 2)
    flags = jnp.any(routes_t[:, None, :, :] == local_ids[None, :, None, None], axis=2)
    earlier = jnp.arange(count)[:, None] < jnp.arange(count)[None, :]
    ranks = jnp.einsum(
        "beu,ut->bet",
        flags.astype(jnp.bfloat16),
        earlier.astype(jnp.bfloat16),
        preferred_element_type=jnp.float32,
    ).astype(jnp.int32)
    slot_of = jnp.where(flags & (ranks < capacity), ranks, -1)
    slot_ids = jnp.arange(padded, dtype=jnp.int32)
    chosen_slot = slot_of[:, :, None, :] == slot_ids[None, None, :, None]
    pick = chosen_slot.astype(jnp.bfloat16).reshape(spread, local_experts * padded, count)
    pick = lax.optimization_barrier(pick)

    def to_slots(rows):
        return jnp.einsum(
            "bjt,btd->bjd", pick, rows, preferred_element_type=jnp.float32
        ).astype(jnp.bfloat16).reshape(spread, local_experts, padded, width)

    def from_slots(slots):
        return jnp.einsum(
            "bjt,bjd->btd",
            pick,
            slots.reshape(spread, local_experts * padded, width),
            preferred_element_type=jnp.float32,
        ).reshape(group, width)

    cotangent_slots = to_slots(cotangent_all)

    token_f = tokens.astype(jnp.float32)
    inverse_one = lax.rsqrt(jnp.mean(token_f * token_f, axis=-1, keepdims=True) + norm_eps)
    unit_one = token_f * inverse_one
    normed_one = (unit_one * attn_scale.astype(jnp.float32)).astype(jnp.bfloat16)
    pre = jnp.dot(normed_one, qkv_full, preferred_element_type=jnp.float32)
    query_pre = pre[:, :query_cols].reshape(count, kv_local * ratio, HD)
    key_pre = pre[:, query_cols : query_cols + key_cols].reshape(count, kv_local, HD)
    query_b = (
        rotate(query_pre, cosine, sine).astype(jnp.bfloat16).reshape(count, kv_local, ratio, HD)
    )
    key_b = rotate(key_pre, cosine, sine).astype(jnp.bfloat16).reshape(count, kv_local * HD)
    value_b = pre[:, query_cols + key_cols :].astype(jnp.bfloat16)
    keys_values = lax.all_gather(
        jnp.concatenate([key_b, value_b], axis=1), "ctx", axis=0, tiled=True
    )
    query_heads = jnp.moveaxis(query_b, 1, 0)
    kv_heads = jnp.moveaxis(keys_values.reshape(group, 2 * kv_local, HD), 1, 0)
    key_heads, value_heads = kv_heads[:kv_local], kv_heads[kv_local:]

    def masked_scores(query_one, key_one):
        scores = (
            jnp.einsum("qrd,kd->qrk", query_one, key_one, preferred_element_type=jnp.float32)
            * scale
        )
        return jnp.where(allowed[:, None, :], scores, -1e30)

    def head_forward(operands):
        query_one, key_one, value_one = operands
        scores = masked_scores(query_one, key_one)
        highest = jnp.max(scores, axis=-1, keepdims=True)
        expo = jnp.exp(scores - highest)
        total = jnp.sum(expo, axis=-1, keepdims=True)
        probs = (expo / total).astype(jnp.bfloat16)
        mixed = jnp.einsum("qrk,kd->qrd", probs, value_one, preferred_element_type=jnp.float32)
        return (mixed, highest + jnp.log(total))

    head_out, log_sums = lax.map(head_forward, (query_heads, key_heads, value_heads))
    mixed_b = (
        jnp.moveaxis(head_out, 0, 1).reshape(count, kv_local * ratio * HD).astype(jnp.bfloat16)
    )
    attn_part = jnp.dot(mixed_b, out_full, preferred_element_type=jnp.float32)
    attn_total = lax.psum(attn_part, "tp")
    hidden = token_f + attn_total
    inverse_two = lax.rsqrt(jnp.mean(hidden * hidden, axis=-1, keepdims=True) + norm_eps)
    unit_two = hidden * inverse_two
    normed_two = (unit_two * moe_scale.astype(jnp.float32)).astype(jnp.bfloat16)
    normed_all = gather_spread(normed_two)
    logits = jnp.dot(normed_all, router_full, preferred_element_type=jnp.float32).reshape(
        spread, count, experts
    )
    hits = jnp.any(routes_all[:, :, :, None] == expert_ids, axis=2)
    highest_logit = jnp.max(jnp.where(hits, logits, -jnp.inf), axis=-1, keepdims=True)
    weight = jnp.where(hits, jnp.exp(jnp.where(hits, logits - highest_logit, 0.0)), 0.0)
    gates_all = weight / jnp.sum(weight, axis=-1, keepdims=True)
    gates = lax.dynamic_index_in_dim(gates_all, place, 0, keepdims=False)
    gates_local = jnp.swapaxes(
        lax.dynamic_slice_in_dim(gates_all, first_expert, local_experts, 2), 1, 2
    )
    slot_gate = jnp.sum(
        jnp.where(chosen_slot, gates_local[:, :, None, :], 0.0), axis=-1, keepdims=True
    )
    token_slots = to_slots(normed_all.reshape(spread, count, width))
    both_pre = jnp.einsum(
        "becd,edf->becf", token_slots, gate_up_full, preferred_element_type=jnp.float32
    )
    active_grad = jnp.einsum(
        "becd,edf->becf", cotangent_slots, down_full, preferred_element_type=jnp.float32
    )
    gate_pre, up_pre = both_pre[..., :hidden_units], both_pre[..., hidden_units:]
    sigma = jax.nn.sigmoid(gate_pre)
    silu_gate = gate_pre * sigma
    active = silu_gate * up_pre
    gate_grad_slots = jnp.sum(active * active_grad, axis=-1)
    active_weighted = (slot_gate * active).astype(jnp.bfloat16)
    weighted_grad = slot_gate * active_grad
    up_grad = weighted_grad * silu_gate
    gate_grad = weighted_grad * up_pre * sigma * (1.0 + gate_pre * (1.0 - sigma))
    both_grad = jnp.concatenate([gate_grad, up_grad], axis=-1).astype(jnp.bfloat16)
    active_weighted, both_grad = lax.optimization_barrier((active_weighted, both_grad))
    input_slots = jnp.einsum(
        "becf,edf->becd", both_grad, gate_up_full, preferred_element_type=jnp.float32
    ).astype(jnp.bfloat16)
    normed_grad = sum_to_owner(from_slots(input_slots))
    gate_grad_rows = jnp.swapaxes(
        jnp.sum(jnp.where(chosen_slot, gate_grad_slots[..., None], 0.0), axis=2), 1, 2
    )
    gate_grad_wide = lax.dynamic_update_slice_in_dim(
        jnp.zeros((spread, count, experts), jnp.float32), gate_grad_rows, first_expert, 2
    ).reshape(group, experts)
    gate_grad_own = lax.psum(
        lax.psum_scatter(gate_grad_wide, "ctx", scatter_dimension=0, tiled=True), "tp"
    )
    result_slots = jnp.einsum(
        "becf,edf->becd", active_weighted, down_full, preferred_element_type=jnp.float32
    ).astype(jnp.bfloat16)
    moe_sum = sum_to_owner(from_slots(result_slots))
    output = (hidden + moe_sum).astype(jnp.bfloat16)
    grad_gate_up = jnp.einsum(
        "becd,becf->edf", token_slots, both_grad, preferred_element_type=jnp.float32
    )
    grad_down = jnp.einsum(
        "becd,becf->edf", cotangent_slots, active_weighted, preferred_element_type=jnp.float32
    )
    joined_grad = lax.psum_scatter(
        jnp.concatenate([grad_gate_up, grad_down], axis=2).astype(jnp.bfloat16),
        "fsdp",
        scatter_dimension=1,
        tiled=True,
    ).astype(jnp.float32)

    grad_output = cotangent.astype(jnp.float32)
    logit_grad = (
        gates * (gate_grad_own - jnp.sum(gates * gate_grad_own, axis=-1, keepdims=True))
    ).astype(jnp.bfloat16)
    grad_router = over_rows(normed_two, logit_grad)
    normed_grad = normed_grad + over_cols(logit_grad, router_full)
    grad_moe_gain = jnp.sum(normed_grad * unit_two, axis=0)
    scaled_two = normed_grad * moe_scale.astype(jnp.float32)
    hidden_grad = grad_output + inverse_two * (
        scaled_two - unit_two * jnp.mean(scaled_two * unit_two, axis=-1, keepdims=True)
    )
    hidden_grad_b = hidden_grad.astype(jnp.bfloat16)
    grad_wout = over_rows(hidden_grad_b, mixed_b)
    lanes = 128
    thin = jnp.concatenate(
        [
            grad_router,
            grad_moe_gain[:, None],
            jnp.zeros((width, lanes - 1 - experts), jnp.float32),
        ],
        axis=1,
    )
    early = lax.psum_scatter(
        jnp.concatenate([grad_wout, thin], axis=1).astype(jnp.bfloat16),
        ("fsdp", "ctx"),
        scatter_dimension=0,
        tiled=True,
    ).astype(jnp.float32)
    out_rows = grad_wout.shape[1]
    mixed_grad = over_cols(hidden_grad_b, out_full).astype(jnp.bfloat16)
    mixed_heads = jnp.moveaxis(mixed_grad.reshape(count, kv_local, ratio, HD), 1, 0)

    def head_backward(operands):
        query_one, key_one, value_one, grad_one, log_sum = operands
        probs = jnp.exp(masked_scores(query_one, key_one) - log_sum)
        probs_b = probs.astype(jnp.bfloat16)
        prob_grad = jnp.einsum(
            "qrd,kd->qrk", grad_one, value_one, preferred_element_type=jnp.float32
        )
        value_grad = jnp.einsum(
            "qrk,qrd->kd", probs_b, grad_one, preferred_element_type=jnp.float32
        )
        delta = jnp.sum(probs * prob_grad, axis=-1, keepdims=True)
        score_grad = (probs * (prob_grad - delta) * scale).astype(jnp.bfloat16)
        query_grad = jnp.einsum(
            "qrk,kd->qrd", score_grad, key_one, preferred_element_type=jnp.float32
        )
        key_grad = jnp.einsum(
            "qrk,qrd->kd", score_grad, query_one, preferred_element_type=jnp.float32
        )
        return (query_grad, key_grad, value_grad)

    query_grads, key_grads, value_grads = lax.map(
        head_backward, (query_heads, key_heads, value_heads, mixed_heads, log_sums)
    )
    kv_terms = jnp.moveaxis(jnp.concatenate([key_grads, value_grads], axis=0), 0, 1).reshape(
        group, 2 * kv_local * HD
    )
    kv_sum = lax.psum_scatter(
        kv_terms.astype(jnp.bfloat16), "ctx", scatter_dimension=0, tiled=True
    ).astype(jnp.float32)
    key_sum, value_sum = kv_sum[:, :key_cols], kv_sum[:, key_cols:]
    key_grad_b = (
        rotate(key_sum.reshape(count, kv_local, HD), cosine, -sine)
        .reshape(count, kv_local * HD)
        .astype(jnp.bfloat16)
    )
    value_grad_b = value_sum.astype(jnp.bfloat16)
    query_grad_b = (
        rotate(jnp.moveaxis(query_grads, 0, 1).reshape(count, kv_local * ratio, HD), cosine, -sine)
        .reshape(count, kv_local * ratio * HD)
        .astype(jnp.bfloat16)
    )
    qkv_grad_b = jnp.concatenate([query_grad_b, key_grad_b, value_grad_b], axis=1)
    normed_one_part = over_cols(qkv_grad_b, qkv_full)
    normed_one_grad = lax.psum(normed_one_part.astype(jnp.bfloat16), "tp").astype(jnp.float32)
    grad_attn_gain = jnp.sum(normed_one_grad * unit_one, axis=0)
    grad_qkv = over_rows(normed_one, qkv_grad_b)
    late = lax.psum_scatter(
        jnp.concatenate([grad_qkv, jnp.broadcast_to(grad_attn_gain[:, None], (width, lanes))], axis=1).astype(jnp.bfloat16),
        ("fsdp", "ctx"),
        scatter_dimension=0,
        tiled=True,
    ).astype(jnp.float32)
    scaled_one = normed_one_grad * attn_scale.astype(jnp.float32)
    token_grad = hidden_grad + inverse_one * (
        scaled_one - unit_one * jnp.mean(scaled_one * unit_one, axis=-1, keepdims=True)
    )
    return (
        output,
        token_grad,
        late[:, query_cols + 2 * key_cols],
        early[:, out_rows + experts],
        late[:, :query_cols],
        late[:, query_cols : query_cols + key_cols],
        late[:, query_cols + key_cols : query_cols + 2 * key_cols],
        early[:, :out_rows].T,
        early[:, out_rows : out_rows + experts],
        joined_grad[:, :, :hidden_units],
        joined_grad[:, :, hidden_units : 2 * hidden_units],
        jnp.swapaxes(joined_grad[:, :, 2 * hidden_units :], 1, 2),
    )


def solution(mesh):
    return jax.shard_map(
        on_device,
        mesh=mesh,
        in_specs=(
            P(("fsdp", "ctx"), None),
            P(("fsdp", "ctx"), None),
            P(("fsdp", "ctx"), None),
            P("fsdp"),
            P("fsdp"),
            P("fsdp", "tp"),
            P("fsdp", "tp"),
            P("fsdp", "tp"),
            P("tp", "fsdp"),
            P("fsdp", None),
            P("ctx", "fsdp", "tp"),
            P("ctx", "fsdp", "tp"),
            P("ctx", "tp", "fsdp"),
        ),
        out_specs=(
            P(("fsdp", "ctx"), None),
            P(("fsdp", "ctx"), None),
            P(("fsdp", "ctx")),
            P(("fsdp", "ctx")),
            P(("fsdp", "ctx"), "tp"),
            P(("fsdp", "ctx"), "tp"),
            P(("fsdp", "ctx"), "tp"),
            P("tp", ("fsdp", "ctx")),
            P(("fsdp", "ctx"), None),
            P("ctx", "fsdp", "tp"),
            P("ctx", "fsdp", "tp"),
            P("ctx", "tp", "fsdp"),
        ),
        check_vma=False,
    )
```
